32 devices in a mesh: freq: 8 (over z, core), plane: 4 (over y, x).
Axes of the slice: x: 2, y: 2, z: 4, core: 2. Of those that a mesh axis runs over, the one named last changes fastest.
Arguments:
- contrast: float32 [2, 512, 2, 512], P(None, 'plane'), may hold values from -1 to 1
- green_kernel: bfloat16 [8, 2, 2, 2, 512, 512], P('freq', None, None, None, 'plane'), may hold values from -1 to 1
- source_pos: int32 [8, 2], P('freq'), may hold values from 0 to 511
- receiver_pos: int32 [8, 2, 64], P('freq'), may hold values from 0 to 511
- measured: float32 [8, 2, 64], P('freq'), may hold values from -6 to 6
Outputs:
- new_contrast: float32 [2, 512, 2, 512], P(None, 'plane')
- new_field: float32 [8, 2, 512, 2, 512], P('freq', None, 'plane')
The draws below stay inside these ranges and needn't reach their ends.
Inputs may be any that keep to these rules, and one draw needn't show every extreme that they name: `source_pos`: row 0 is the x index and row 1 the y index of the source cell in layer 0. `receiver_pos`: row 0 holds the x indices and row 1 the y indices of the receiver cells in layer 0; receivers may coincide.
All inputs are finite; a program needn't handle non-finite values.
Results may differ from the reference program's by a relative error of at most 0.02.
Values may be sent and summed in bfloat16 or wider, within the bound.
A program may use at most 64 MiB of HBM per device.

```python
import math
import jax
import jax.numpy as jnp
from jax import lax

GRID = 512
LAYERS = 2
ITERS = 2
RECV = 64
FREQS = 8


def set_ends(array, stream_key, smallest, high):
    shape = array.shape
    place = [jax.random.randint(jax.random.fold_in(stream_key, axis), (), 0, shape[axis]) for axis in range(len(shape))]
    array = array.at[tuple(place)].set(smallest)
    longest = shape.index(max(shape))
    place[longest] = (place[longest] + 1) % shape[longest]
    return array.at[tuple(place)].set(high)


def block_levels(stream_key, extent, split, low, high):
    gain = 1.0
    for axis_at, shards_of in split:
        draws = jax.random.uniform(jax.random.fold_in(jax.random.fold_in(stream_key, 6), axis_at), (shards_of,), jnp.float32, low / len(split), high / len(split))
        gain = gain * jnp.repeat(jnp.exp(draws), extent[axis_at] // shards_of).reshape((-1,) + (1,) * (len(extent) - 1 - axis_at))
    return gain


def scatter_about(stream_key, extent, spread, reach, pieces=(), held_as=jnp.bfloat16):
    factor_of = block_levels(stream_key, extent, pieces, -0.22, 0.18) if pieces else 1.0
    values = jax.random.normal(stream_key, extent, jnp.float32) * spread * factor_of
    return jnp.minimum(jnp.maximum(values, -reach), reach).astype(held_as)


def setup_inputs(seed: int = 0) -> dict:
    key_list = jax.random.split(jax.random.key(seed), 6)
    contrast = jnp.clip(jax.random.uniform(key_list[0], (2, GRID, LAYERS, GRID), jnp.float32, -1.0, 1.0) * block_levels(key_list[0], (2, GRID, LAYERS, GRID), ((1, 4),), -0.4, 0.0), -1.0, 1.0)
    green_kernel = scatter_about(key_list[1], (FREQS, 2, LAYERS, LAYERS, GRID, GRID), 0.25, 1.0, ((0, 8), (4, 4)))
    source_pos = set_ends(jax.random.randint(key_list[2], (FREQS, 2), 0, GRID), jax.random.fold_in(key_list[2], 1), 0, GRID - 1).astype(jnp.int32)
    receiver_pos = set_ends(jax.random.randint(key_list[3], (FREQS, 2, RECV), 0, GRID), jax.random.fold_in(key_list[3], 1), 0, GRID - 1).astype(jnp.int32)
    measured = scatter_about(key_list[4], (FREQS, 2, RECV), 1.0, 6.0, ((0, 8),), jnp.float32)
    return {"contrast": contrast, "green_kernel": green_kernel, "source_pos": source_pos, "receiver_pos": receiver_pos, "measured": measured}


source_gain = 3.0

def to_half(values):
    return lax.optimization_barrier(values.astype(jnp.bfloat16)).astype(jnp.float32)

def matmul_hi(left, right):
    return jnp.dot(left, right, precision=lax.Precision.HIGHEST, preferred_element_type=jnp.float32)

def make_tables(length):
    positions = jnp.arange(length, dtype=jnp.int32)
    turn_count = positions[:, None] * positions[None, :] % length
    angles = turn_count.astype(jnp.float32) * (2.0 * math.pi / length)
    norm_scale = 1.0 / math.sqrt(length)
    return (to_half(jnp.cos(angles) * norm_scale), to_half(jnp.sin(angles) * norm_scale))

def line_phase(positions, location, length):
    turn_count = positions * location % length
    angles = turn_count.astype(jnp.float32) * (2.0 * math.pi / length)
    return (jnp.cos(angles), -jnp.sin(angles))

def forward(field_real, field_imag, cos_table, sin_table):
    grid_size, layer_count, _ = field_real.shape
    in_real = to_half(field_real).reshape(grid_size * layer_count, grid_size)
    in_imag = to_half(field_imag).reshape(grid_size * layer_count, grid_size)
    mid_real = to_half(matmul_hi(in_real, cos_table) + matmul_hi(in_imag, sin_table)).reshape(grid_size, layer_count * grid_size)
    mid_imag = to_half(matmul_hi(in_imag, cos_table) - matmul_hi(in_real, sin_table)).reshape(grid_size, layer_count * grid_size)
    out_real = matmul_hi(mid_real.T, cos_table) + matmul_hi(mid_imag.T, sin_table)
    out_imag = matmul_hi(mid_imag.T, cos_table) - matmul_hi(mid_real.T, sin_table)
    return (out_real.reshape(layer_count, grid_size, grid_size), out_imag.reshape(layer_count, grid_size, grid_size))

def inverse(spec_real, spec_imag, cos_table, sin_table):
    layer_count, grid_size, _ = spec_real.shape
    in_real = to_half(spec_real).reshape(layer_count * grid_size, grid_size)
    in_imag = to_half(spec_imag).reshape(layer_count * grid_size, grid_size)
    mid_real = to_half(matmul_hi(in_real, cos_table) - matmul_hi(in_imag, sin_table))
    mid_imag = to_half(matmul_hi(in_imag, cos_table) + matmul_hi(in_real, sin_table))
    mid_real = mid_real.T.reshape(grid_size * layer_count, grid_size)
    mid_imag = mid_imag.T.reshape(grid_size * layer_count, grid_size)
    out_real = matmul_hi(mid_real, cos_table) - matmul_hi(mid_imag, sin_table)
    out_imag = matmul_hi(mid_imag, cos_table) + matmul_hi(mid_real, sin_table)
    return (out_real.reshape(grid_size, layer_count, grid_size), out_imag.reshape(grid_size, layer_count, grid_size))

def couple(kern_real, kern_imag, spec_real, spec_imag):
    high = lax.Precision.HIGHEST
    out_real = jnp.einsum('lmqk,mqk->lqk', kern_real, spec_real, precision=high) - jnp.einsum('lmqk,mqk->lqk', kern_imag, spec_imag, precision=high)
    out_imag = jnp.einsum('lmqk,mqk->lqk', kern_real, spec_imag, precision=high) + jnp.einsum('lmqk,mqk->lqk', kern_imag, spec_real, precision=high)
    return (out_real, out_imag)

def green_apply(kern_real, kern_imag, field_real, field_imag, cos_table, sin_table):
    spec_real, spec_imag = forward(field_real, field_imag, cos_table, sin_table)
    spec_real, spec_imag = couple(kern_real, kern_imag, spec_real, spec_imag)
    return inverse(spec_real, spec_imag, cos_table, sin_table)

def reference(contrast, green_kernel, source_pos, receiver_pos, measured):
    grid_size = contrast.shape[3]
    cos_table, sin_table = make_tables(grid_size)
    con_real = contrast[0]
    con_imag = contrast[1]
    positions = jnp.arange(grid_size, dtype=jnp.int32)

    def one_freq(carry, inputs):
        grad_real, grad_imag = carry
        kernel, source, receivers, observed = inputs
        kern_real = kernel[0].astype(jnp.float32)
        kern_imag = kernel[1].astype(jnp.float32)
        phase_y_real, phase_y_imag = line_phase(positions, source[1], grid_size)
        phase_x_real, phase_x_imag = line_phase(positions, source[0], grid_size)
        source_real = source_gain * (phase_y_real[:, None] * phase_x_real[None, :] - phase_y_imag[:, None] * phase_x_imag[None, :])
        source_imag = source_gain * (phase_y_real[:, None] * phase_x_imag[None, :] + phase_y_imag[:, None] * phase_x_real[None, :])
        spec_real = kern_real[:, 0] * source_real - kern_imag[:, 0] * source_imag
        spec_imag = kern_real[:, 0] * source_imag + kern_imag[:, 0] * source_real
        inc_real, inc_imag = inverse(spec_real, spec_imag, cos_table, sin_table)
        wave_real, wave_imag = (inc_real, inc_imag)
        for sweep_index in range(ITERS):
            prod_real = con_real * wave_real - con_imag * wave_imag
            prod_imag = con_real * wave_imag + con_imag * wave_real
            delta_real, delta_imag = green_apply(kern_real, kern_imag, prod_real, prod_imag, cos_table, sin_table)
            wave_real = inc_real + delta_real
            wave_imag = inc_imag + delta_imag
        misfit_real = wave_real[receivers[0], 0, receivers[1]] - observed[0]
        misfit_imag = wave_imag[receivers[0], 0, receivers[1]] - observed[1]
        recv_y_real, recv_y_imag = line_phase(positions[None, :], receivers[1][:, None], grid_size)
        recv_x_real, recv_x_imag = line_phase(positions[None, :], receivers[0][:, None], grid_size)
        mixed_real = misfit_real[:, None] * recv_y_real - misfit_imag[:, None] * recv_y_imag
        mixed_imag = misfit_real[:, None] * recv_y_imag + misfit_imag[:, None] * recv_y_real
        adj_real = matmul_hi(mixed_real.T, recv_x_real) - matmul_hi(mixed_imag.T, recv_x_imag)
        adj_imag = matmul_hi(mixed_real.T, recv_x_imag) + matmul_hi(mixed_imag.T, recv_x_real)
        back_spec_real = kern_real[0] * adj_real + kern_imag[0] * adj_imag
        back_spec_imag = kern_real[0] * adj_imag - kern_imag[0] * adj_real
        back_real, back_imag = inverse(back_spec_real, back_spec_imag, cos_table, sin_table)
        grad_real = grad_real + (wave_real * back_real + wave_imag * back_imag)
        grad_imag = grad_imag + (wave_real * back_imag - wave_imag * back_real)
        return ((grad_real, grad_imag), (inc_real, inc_imag, wave_real, wave_imag))
    zero_grad = jnp.zeros(con_real.shape, jnp.float32)
    (grad_real, grad_imag), kept = lax.scan(one_freq, (zero_grad, zero_grad), (green_kernel, source_pos, receiver_pos, measured))
    new_real = con_real - grad_real / FREQS
    new_imag = con_imag - grad_imag / FREQS

    def final(inputs):
        kernel, inc_real, inc_imag, wave_real, wave_imag = inputs
        kern_real = kernel[0].astype(jnp.float32)
        kern_imag = kernel[1].astype(jnp.float32)
        prod_real = new_real * wave_real - new_imag * wave_imag
        prod_imag = new_real * wave_imag + new_imag * wave_real
        delta_real, delta_imag = green_apply(kern_real, kern_imag, prod_real, prod_imag, cos_table, sin_table)
        return jnp.stack([inc_real + delta_real, inc_imag + delta_imag])
    new_field = lax.map(final, (green_kernel,) + tuple(kept))
    return (jnp.stack([new_real, new_imag]), new_field)
```

```python
import functools
import math

import jax
import numpy as np
import jax.numpy as jnp
from jax import lax
from jax.experimental import pallas as pl
from jax.experimental.pallas import tpu as pltpu
from jax.sharding import PartitionSpec as P

ITERS = 2


source_gain = 3.0


def phase_tables(length, out_type):
    positions = lax.iota(jnp.int32, length)
    turn_count = positions[:, None] * positions[None, :] % length
    angles = turn_count.astype(jnp.float32) * (2.0 * math.pi / length)
    norm_scale = 1.0 / math.sqrt(length)
    return jnp.concatenate(
        [jnp.cos(angles) * norm_scale, jnp.sin(angles) * norm_scale], axis=1
    ).astype(out_type)


def line_phase(positions, location, length):
    turn_count = positions * location % length
    angles = turn_count.astype(jnp.float32) * (2.0 * math.pi / length)
    return (jnp.cos(angles), -jnp.sin(angles))


def complex_product(first, second):
    return jnp.stack(
        [first[0] * second[0] - first[1] * second[1], first[0] * second[1] + first[1] * second[0]]
    )


def forward(wave_field, dft_table):
    row_count, layer_count, grid_size = wave_field.shape[1:]
    narrowed = wave_field.astype(jnp.bfloat16)
    products = jnp.dot(
        narrowed.reshape(2 * row_count * layer_count, grid_size),
        dft_table,
        preferred_element_type=jnp.float32,
    )
    products = products.reshape(2, row_count, layer_count, 2, grid_size)
    real_part = products[0, :, :, 0] + products[1, :, :, 1]
    imag_part = products[1, :, :, 0] - products[0, :, :, 1]
    narrowed = jnp.stack([real_part, imag_part]).astype(jnp.bfloat16)
    arrived = lax.all_to_all(narrowed, "plane", split_axis=3, concat_axis=1, tiled=True)
    col_count = arrived.shape[3]
    merged = arrived.reshape(2, grid_size, layer_count * col_count)
    products = jnp.einsum("cxq,xk->cqk", merged, dft_table, preferred_element_type=jnp.float32)
    real_part = products[0, :, :grid_size] + products[1, :, grid_size:]
    imag_part = products[1, :, :grid_size] - products[0, :, grid_size:]
    return jnp.stack([real_part, imag_part]).reshape(2, layer_count, col_count, grid_size)


def inverse(spectrum, dft_table):
    layer_count, col_count, grid_size = spectrum.shape[1:]
    narrowed = spectrum.astype(jnp.bfloat16).reshape(2, layer_count * col_count, grid_size)
    products = jnp.einsum("cqk,kt->ctq", narrowed, dft_table, preferred_element_type=jnp.float32)
    real_part = products[0, :grid_size] - products[1, grid_size:]
    imag_part = products[1, :grid_size] + products[0, grid_size:]
    narrowed = (
        jnp.stack([real_part, imag_part])
        .astype(jnp.bfloat16)
        .reshape(2, grid_size, layer_count, col_count)
    )
    arrived = lax.all_to_all(narrowed, "plane", split_axis=1, concat_axis=3, tiled=True)
    row_count = arrived.shape[1]
    products = jnp.dot(
        arrived.reshape(2 * row_count * layer_count, grid_size),
        dft_table,
        preferred_element_type=jnp.float32,
    )
    products = products.reshape(2, row_count, layer_count, 2, grid_size)
    real_part = products[0, :, :, 0] - products[1, :, :, 1]
    imag_part = products[1, :, :, 0] + products[0, :, :, 1]
    return jnp.stack([real_part, imag_part])


def couple(spectrum, kernel):
    layer_count = spectrum.shape[1]
    real_rows = []
    imag_rows = []
    for out_layer in range(layer_count):
        sum_real = jnp.zeros(spectrum.shape[2:], jnp.float32)
        sum_imag = jnp.zeros(spectrum.shape[2:], jnp.float32)
        for in_layer in range(layer_count):
            kern_real = kernel[0, out_layer, in_layer].astype(jnp.float32)
            kern_imag = kernel[1, out_layer, in_layer].astype(jnp.float32)
            sum_real = (
                sum_real + kern_real * spectrum[0, in_layer] - kern_imag * spectrum[1, in_layer]
            )
            sum_imag = (
                sum_imag + kern_real * spectrum[1, in_layer] + kern_imag * spectrum[0, in_layer]
            )
        real_rows.append(sum_real)
        imag_rows.append(sum_imag)
    return jnp.stack([jnp.stack(real_rows), jnp.stack(imag_rows)])


def green_apply(wave_field, kernel, dft_table):
    return inverse(couple(forward(wave_field, dft_table), kernel), dft_table)


def plain_local(contrast, green_kernel, source_pos, receiver_pos, measured):
    freq_count = green_kernel.shape[0]
    row_count = contrast.shape[1]
    grid_size = contrast.shape[3]
    high = lax.Precision.HIGHEST
    dft_table = phase_tables(grid_size, jnp.bfloat16)
    first_row = lax.axis_index("plane") * row_count
    own_rows = first_row + lax.iota(jnp.int32, row_count)
    all_cols = lax.iota(jnp.int32, grid_size)
    which = 0
    kernel = green_kernel[which]
    phase_y_real, phase_y_imag = line_phase(own_rows, source_pos[which, 1], grid_size)
    phase_x_real, phase_x_imag = line_phase(all_cols, source_pos[which, 0], grid_size)
    source_real = source_gain * (
        phase_y_real[:, None] * phase_x_real[None, :]
        - phase_y_imag[:, None] * phase_x_imag[None, :]
    )
    source_imag = source_gain * (
        phase_y_real[:, None] * phase_x_imag[None, :]
        + phase_y_imag[:, None] * phase_x_real[None, :]
    )
    column_zero = kernel[:, :, 0].astype(jnp.float32)
    spectrum = jnp.stack(
        [
            column_zero[0] * source_real - column_zero[1] * source_imag,
            column_zero[0] * source_imag + column_zero[1] * source_real,
        ]
    )
    incident = inverse(spectrum, dft_table)
    wave_field = incident
    for sweep_index in range(ITERS):
        wave_field = incident + green_apply(
            complex_product(contrast, wave_field), kernel, dft_table
        )
    recv_x = receiver_pos[which, 0]
    recv_y = receiver_pos[which, 1]
    pick_rows = (recv_x[:, None] == own_rows[None, :]).astype(jnp.float32)
    pick_cols = (recv_y[:, None] == all_cols[None, :]).astype(jnp.float32)
    surface = jnp.einsum("rx,cxy->cry", pick_rows, wave_field[:, :, 0, :], precision=high)
    sampled = jnp.sum(surface * pick_cols[None], axis=2)
    gathered = lax.psum(sampled, "plane")
    misfit = gathered - measured[which]
    recv_y_real, recv_y_imag = line_phase(own_rows[None, :], recv_y[:, None], grid_size)
    recv_x_real, recv_x_imag = line_phase(all_cols[None, :], recv_x[:, None], grid_size)
    mixed_real = misfit[0][:, None] * recv_y_real - misfit[1][:, None] * recv_y_imag
    mixed_imag = misfit[0][:, None] * recv_y_imag + misfit[1][:, None] * recv_y_real
    contract = (((0,), (0,)), ((), ()))
    adj_real = lax.dot_general(
        mixed_real, recv_x_real, contract, precision=high, preferred_element_type=jnp.float32
    ) - lax.dot_general(
        mixed_imag, recv_x_imag, contract, precision=high, preferred_element_type=jnp.float32
    )
    adj_imag = lax.dot_general(
        mixed_real, recv_x_imag, contract, precision=high, preferred_element_type=jnp.float32
    ) + lax.dot_general(
        mixed_imag, recv_x_real, contract, precision=high, preferred_element_type=jnp.float32
    )
    row_zero = kernel[:, 0].astype(jnp.float32)
    back_spec = jnp.stack(
        [
            row_zero[0] * adj_real + row_zero[1] * adj_imag,
            row_zero[0] * adj_imag - row_zero[1] * adj_real,
        ]
    )
    backward = inverse(back_spec, dft_table)
    gradient = jnp.stack(
        [
            wave_field[0] * backward[0] + wave_field[1] * backward[1],
            wave_field[0] * backward[1] - wave_field[1] * backward[0],
        ]
    )
    incidents = [incident]
    solutions = [wave_field]
    total_freqs = freq_count * lax.axis_size("freq")
    summed = lax.psum(gradient.astype(jnp.bfloat16), "freq").astype(jnp.float32)
    updated = contrast - summed / total_freqs
    which = 0
    outputs = [
        incidents[which]
        + green_apply(complex_product(updated, solutions[which]), green_kernel[which], dft_table)
    ]
    return (updated, jnp.stack(outputs))


HIGH = lax.Precision.HIGHEST


def fused_kernel(
    cfg, con, kt, cos_t, sin_t, src, rx, ry_real, ry_imag, pick_x, pick_y, meas,
    new_con, new_field,
    tab_a, tab_b, inc, wave, back, vb, spec, hb, send_buf, recv_buf,
    samp_out, samp_in, grad, grad_b, half_in, part_out, part_in, total_b,
    send_sem, recv_sem, samp_send, samp_recv,
    one_send, one_recv, two_send, two_recv, three_send, three_recv, four_send, four_recv,
):
    n, nf, ck, layers = cfg
    wide = 2 * ck
    nz = nf // 2
    me = lax.axis_index("plane")
    fr = lax.axis_index("freq")
    core = fr % 2
    z = fr // 2
    mate = fr + 1 - 2 * core

    def peer(k):
        if n == 4:
            return ((me // 2 + k // 2) % 2) * 2 + (me % 2 + k % 2) % 2
        return (me + k) % n

    def source(k):
        return peer(k) if n == 4 else (me + n - k) % n

    order = [3, 1, 2] if n == 4 else list(range(1, n))
    arrive = [1, 2, 3] if n == 4 else list(range(1, n))
    z_peers = [((z + 1 + j) % nz) * 2 + core for j in range(nz - 1)]

    barrier = pltpu.get_barrier_semaphore()
    for k in range(1, n):
        pl.semaphore_signal(barrier, inc=1, device_id={"plane": peer(k)})
    for dev in z_peers + [mate]:
        pl.semaphore_signal(barrier, inc=1, device_id={"freq": dev})

    def remote(src_ref, dst_ref, s, r, where):
        return pltpu.make_async_remote_copy(
            src_ref=src_ref, dst_ref=dst_ref, send_sem=s, recv_sem=r, device_id=where
        )

    def block(i):
        return pl.ds(pl.multiple_of(i * wide, wide), wide)

    def move(ph, k):
        return remote(
            send_buf.at[ph, k], recv_buf.at[ph, k], send_sem.at[ph, k], recv_sem.at[ph, k],
            {"plane": peer(k)},
        )

    for a in range(n):
        for b in range(n):
            cb = cos_t[a * ck : (a + 1) * ck, b * ck : (b + 1) * ck]
            sb = sin_t[a * ck : (a + 1) * ck, b * ck : (b + 1) * ck]
            r0, c0 = a * wide, b * wide
            for tab, up, down in ((tab_a, -sb, sb), (tab_b, sb, -sb)):
                tab[r0 : r0 + ck, c0 : c0 + ck] = cb
                tab[r0 : r0 + ck, c0 + ck : c0 + wide] = up
                tab[r0 + ck : r0 + wide, c0 : c0 + ck] = down
                tab[r0 + ck : r0 + wide, c0 + ck : c0 + wide] = cb

    def dot(a, b):
        return jnp.dot(a, b, preferred_element_type=jnp.float32)

    def forward(ph):
        def piece(d):
            w = dot(vb[...], tab_a[:, block(d)]).astype(jnp.bfloat16)
            return [
                (c, l, w[l * ck : (l + 1) * ck, c * ck : (c + 1) * ck])
                for c in range(2)
                for l in range(layers)
            ]

        for k in order:
            for c, l, w in piece(peer(k)):
                send_buf[ph, k, c * ck : (c + 1) * ck, l * ck : (l + 1) * ck] = w
            move(ph, k).start()
        for c, l, w in piece(me):
            recv_buf[ph, 0, c * ck : (c + 1) * ck, l * ck : (l + 1) * ck] = w
        spec[...] = dot(tab_b[:, block(me)], recv_buf[ph, 0])
        for k in arrive:
            move(ph, k).wait_recv()
            spec[...] += dot(tab_b[:, block(source(k))], recv_buf[ph, k])
        for k in arrive:
            move(ph, k).wait_send()

    def inverse(ph, dst, base):
        for k in order:
            send_buf[ph, k] = dot(tab_a[block(peer(k)), :], hb[...]).astype(jnp.bfloat16)
            move(ph, k).start()
        recv_buf[ph, 0] = dot(tab_a[block(me), :], hb[...]).astype(jnp.bfloat16)

        def part(k, s):
            p = recv_buf[ph, k]
            lhs = jnp.concatenate(
                [
                    jnp.concatenate(
                        [p[:ck, l * ck : (l + 1) * ck], p[ck:, l * ck : (l + 1) * ck]], axis=1
                    )
                    for l in range(layers)
                ],
                axis=0,
            )
            return dot(lhs, tab_b[block(s), :])

        dst[...] = part(0, me) if base is None else base[...] + part(0, me)
        for k in arrive:
            move(ph, k).wait_recv()
            dst[...] += part(k, source(k))
        for k in arrive:
            move(ph, k).wait_send()

    def multiply(contrast_ref):
        for d in range(n):
            lo = slice(d * wide, d * wide + ck)
            hi = slice(d * wide + ck, (d + 1) * wide)
            a_r, a_i = contrast_ref[:, lo], contrast_ref[:, hi]
            u_r, u_i = wave[:, lo], wave[:, hi]
            vb[:, lo] = (a_r * u_r - a_i * u_i).astype(jnp.bfloat16)
            vb[:, hi] = (a_r * u_i + a_i * u_r).astype(jnp.bfloat16)

    def kern(c, lo, li, g):
        return kt[c, lo, li, g * ck : (g + 1) * ck, :].astype(jnp.float32)

    def put(g, l, real, imag):
        lanes = slice(l * ck, (l + 1) * ck)
        hb[g * wide : g * wide + ck, lanes] = real.astype(jnp.bfloat16)
        hb[g * wide + ck : (g + 1) * wide, lanes] = imag.astype(jnp.bfloat16)

    def couple():
        for g in range(n):
            for lo in range(layers):
                real = imag = None
                for li in range(layers):
                    lanes = slice(li * ck, (li + 1) * ck)
                    f_r = spec[g * wide : g * wide + ck, lanes]
                    f_i = spec[g * wide + ck : (g + 1) * wide, lanes]
                    k_r, k_i = kern(0, lo, li, g), kern(1, lo, li, g)
                    add_r = k_r * f_r - k_i * f_i
                    add_i = k_r * f_i + k_i * f_r
                    real = add_r if real is None else real + add_r
                    imag = add_i if imag is None else imag + add_i
                put(g, lo, real, imag)

    for g in range(n):
        q_r, q_i = src[0, g * ck : (g + 1) * ck, :], src[1, g * ck : (g + 1) * ck, :]
        for l in range(layers):
            k_r, k_i = kern(0, l, 0, g), kern(1, l, 0, g)
            put(g, l, k_r * q_r - k_i * q_i, k_r * q_i + k_i * q_r)

    pl.semaphore_wait(barrier, n - 1 + nz)

    inverse(0, inc, None)
    wave[...] = inc[...]

    def sweep(it, carry):
        multiply(con)
        forward(1 + 2 * it)
        couple()
        inverse(2 + 2 * it, wave, inc)
        return carry

    lax.fori_loop(0, ITERS, sweep, 0)
    ph = 1 + 2 * ITERS

    rows = jnp.dot(pick_x[...], wave[:ck, :], precision=HIGH, preferred_element_type=jnp.float32)
    got_r = got_i = None
    for d in range(n):
        mask = pick_y[:, d * ck : (d + 1) * ck]
        s_r = rows[:, d * wide : d * wide + ck] * mask
        s_i = rows[:, d * wide + ck : (d + 1) * wide] * mask
        got_r = s_r if d == 0 else got_r + s_r
        got_i = s_i if d == 0 else got_i + s_i
    got_r = jnp.sum(got_r, axis=1, keepdims=True)
    got_i = jnp.sum(got_i, axis=1, keepdims=True)
    lane = lax.broadcasted_iota(jnp.int32, samp_out.shape, 1)
    half = samp_out.shape[1] // 2
    samp_out[...] = jnp.where(lane < half, got_r, got_i)

    def tell(k):
        return remote(
            samp_out, samp_in.at[k], samp_send.at[k], samp_recv.at[k], {"plane": peer(k)}
        )

    for k in order:
        tell(k).start()
    misfit = samp_out[...] - meas[...]
    for k in arrive:
        tell(k).wait_recv()
        misfit = misfit + samp_in[k]
    for k in arrive:
        tell(k).wait_send()
    m_r = misfit[:, 0:1]
    m_i = misfit[:, half : half + 1]
    y_r, y_i = ry_real[...], ry_imag[...]
    mixed = jnp.concatenate([m_r * y_r - m_i * y_i, m_r * y_i + m_i * y_r], axis=0)
    for g in range(n):
        adj = jnp.dot(
            rx[g * wide : (g + 1) * wide, :], mixed,
            precision=HIGH, preferred_element_type=jnp.float32,
        )
        a_r, a_i = adj[:ck], adj[ck:]
        for l in range(layers):
            k_r, k_i = kern(0, 0, l, g), kern(1, 0, l, g)
            put(g, l, k_r * a_r + k_i * a_i, k_r * a_i - k_i * a_r)
    inverse(ph, back, None)

    for d in range(n):
        lo = slice(d * wide, d * wide + ck)
        hi = slice(d * wide + ck, (d + 1) * wide)
        b_r, b_i, u_r, u_i = back[:, lo], back[:, hi], wave[:, lo], wave[:, hi]
        g_r = u_r * b_r + u_i * b_i
        g_i = u_r * b_i - u_i * b_r
        grad[:, lo] = g_r
        grad[:, hi] = g_i
        grad_b[:, lo] = g_r.astype(jnp.bfloat16)
        grad_b[:, hi] = g_i.astype(jnp.bfloat16)

    height = grad.shape[0] // 2
    q = height // nz

    def span(c, i):
        return pl.ds(pl.multiple_of(c * height + i * q, q), q)

    def first(j):
        t = (z + 1 + j) % nz
        return remote(
            grad_b.at[span(1 - core, t), :], half_in.at[j],
            one_send.at[j], one_recv.at[j], {"freq": mate},
        )

    def second(j):
        return remote(
            part_out.at[j], part_in.at[j], two_send.at[j], two_recv.at[j], {"freq": z_peers[j]}
        )

    for j in range(nz):
        first(j).start()
    mine = None
    for j in range(nz):
        t = (z + 1 + j) % nz
        first(j).wait_recv()
        mine = grad[span(core, t), :] + half_in[j].astype(jnp.float32)
        if j < nz - 1:
            part_out[j] = mine.astype(jnp.bfloat16)
            second(j).start()
    for j in range(nz - 1):
        second(j).wait_recv()
        mine = mine + part_in[j].astype(jnp.float32)
    total_b[span(core, z), :] = mine.astype(jnp.bfloat16)

    def third(j, i):
        rows_at = total_b.at[span(core, i), :]
        return remote(rows_at, rows_at, three_send.at[j], three_recv.at[j], {"freq": z_peers[j]})

    def fourth(j, c, i):
        rows_at = total_b.at[span(c, i), :]
        return remote(rows_at, rows_at, four_send.at[j], four_recv.at[j], {"freq": mate})

    for j in range(nz - 1):
        third(j, z).start()
    fourth(nz - 1, core, z).start()
    froms = [(z + nz - 1 - j) % nz for j in range(nz - 1)] + [z]
    for j in range(nz - 1):
        third(j, froms[j]).wait_recv()
        fourth(j, core, froms[j]).start()
    for j in reversed(range(nz)):
        fourth(j, 1 - core, froms[j]).wait_recv()
    for j in range(nz):
        first(j).wait_send()
        fourth(j, core, froms[j]).wait_send()
        if j < nz - 1:
            second(j).wait_send()
            third(j, z).wait_send()
    new_con[...] = con[...] - total_b[...].astype(jnp.float32) / nf

    multiply(new_con)
    forward(ph + 1)
    couple()
    inverse(ph + 2, new_field, inc)


def fused_local(contrast, green_kernel, source_pos, receiver_pos, measured):
    _, ck, layers, grid = contrast.shape
    n = lax.axis_size("plane")
    nf = lax.axis_size("freq")
    recv = receiver_pos.shape[2]
    wide = 2 * ck
    pos = np.arange(grid)
    ang = (pos[:, None] * pos[None, :] % grid) * (2.0 * math.pi / grid)
    cos_t = jnp.asarray((np.cos(ang) / math.sqrt(grid)).astype(np.float32).astype(jnp.bfloat16))
    sin_t = jnp.asarray((np.sin(ang) / math.sqrt(grid)).astype(np.float32).astype(jnp.bfloat16))
    own_rows = lax.axis_index("plane") * ck + lax.iota(jnp.int32, ck)
    all_cols = lax.iota(jnp.int32, grid)
    con = contrast.reshape(2, ck, layers, n, ck).transpose(2, 1, 3, 0, 4)
    con = con.reshape(layers * ck, 2 * grid)
    kt = green_kernel[0].transpose(0, 1, 2, 4, 3)
    sy_r, sy_i = line_phase(own_rows, source_pos[0, 1], grid)
    sx_r, sx_i = line_phase(all_cols, source_pos[0, 0], grid)
    src = source_gain * complex_product((sx_r[:, None], sx_i[:, None]), (sy_r[None], sy_i[None]))
    recv_x, recv_y = receiver_pos[0, 0], receiver_pos[0, 1]
    ry_r, ry_i = line_phase(own_rows[None, :], recv_y[:, None], grid)
    rx_r, rx_i = line_phase(all_cols[:, None], recv_x[None, :], grid)
    rx_r, rx_i = rx_r.reshape(n, ck, recv), rx_i.reshape(n, ck, recv)
    rx = jnp.concatenate(
        [jnp.concatenate([rx_r, -rx_i], axis=2), jnp.concatenate([rx_i, rx_r], axis=2)], axis=1
    ).reshape(n * wide, 2 * recv)
    pick_x = (recv_x[:, None] == own_rows[None, :]).astype(jnp.float32)
    pick_y = (recv_y[:, None] == all_cols[None, :]).astype(jnp.float32)
    meas = jnp.repeat(measured[0], 64, axis=0).reshape(2, 64, recv).transpose(2, 0, 1)
    meas = meas.reshape(recv, 128)

    rows, cols, lanes = layers * ck, 2 * grid, layers * ck
    nz = nf // 2
    phases = 2 * ITERS + 4
    f32, bf16 = jnp.float32, jnp.bfloat16
    q = rows // 2 // nz
    dma = pltpu.SemaphoreType.DMA
    vm = pltpu.VMEM
    scratch = [
        vm((cols, cols), bf16), vm((cols, cols), bf16), vm((rows, cols), f32),
        vm((rows, cols), f32), vm((rows, cols), f32), vm((rows, cols), bf16),
        vm((cols, lanes), f32), vm((cols, lanes), bf16),
        vm((phases, n, wide, lanes), bf16), vm((phases, n, wide, lanes), bf16),
        vm((recv, 128), f32), vm((n, recv, 128), f32),
        vm((rows, cols), f32), vm((rows, cols), bf16), vm((nz, q, cols), bf16),
        vm((nz - 1, q, cols), bf16), vm((nz - 1, q, cols), bf16), vm((rows, cols), bf16),
        dma((phases, n)), dma((phases, n)), dma((n,)), dma((n,)),
        dma((nz,)), dma((nz,)), dma((nz - 1,)), dma((nz - 1,)),
        dma((nz - 1,)), dma((nz - 1,)), dma((nz,)), dma((nz,)),
    ]
    spec = pl.BlockSpec(memory_space=pltpu.VMEM)
    new_con, new_field = pl.pallas_call(
        functools.partial(fused_kernel, (n, nf, ck, layers)),
        out_shape=[jax.ShapeDtypeStruct((rows, cols), f32)] * 2,
        in_specs=[spec] * 11,
        out_specs=[spec] * 2,
        scratch_shapes=scratch,
        compiler_params=pltpu.CompilerParams(
            collective_id=0, has_side_effects=True, vmem_limit_bytes=56 * 2**20
        ),
    )(con, kt, cos_t, sin_t, src, rx, ry_r, ry_i, pick_x, pick_y, meas)

    def restore(values):
        values = values.reshape(layers, ck, n, 2, ck).transpose(3, 1, 0, 2, 4)
        return values.reshape(2, ck, layers, grid)

    return restore(new_con), restore(new_field)[None]


def chosen(contrast, green_kernel, source_pos, receiver_pos, measured):
    ck = contrast.shape[1]
    nf = lax.axis_size("freq")
    fits = (
        ck % 128 == 0
        and green_kernel.shape[0] == 1
        and nf % 2 == 0
        and nf >= 4
        and (contrast.shape[2] * ck) % (16 * nf) == 0
        and lax.axis_size("plane") > 1
    )
    body = fused_local if fits else plain_local
    return body(contrast, green_kernel, source_pos, receiver_pos, measured)


def solution(mesh):
    return jax.shard_map(
        chosen,
        mesh=mesh,
        in_specs=(
            P(None, "plane", None, None),
            P("freq", None, None, None, "plane", None),
            P("freq", None),
            P("freq", None, None),
            P("freq", None, None),
        ),
        out_specs=(P(None, "plane", None, None), P("freq", None, "plane", None, None)),
        check_vma=False,
    )
```

```python
import functools
import math

import jax
import numpy as np
import jax.numpy as jnp
from jax import lax
from jax.experimental import pallas as pl
from jax.experimental.pallas import tpu as pltpu
from jax.sharding import PartitionSpec as P

ITERS = 2


source_gain = 3.0


def phase_tables(length, out_type):
    positions = lax.iota(jnp.int32, length)
    turn_count = positions[:, None] * positions[None, :] % length
    angles = turn_count.astype(jnp.float32) * (2.0 * math.pi / length)
    norm_scale = 1.0 / math.sqrt(length)
    return jnp.concatenate(
        [jnp.cos(angles) * norm_scale, jnp.sin(angles) * norm_scale], axis=1
    ).astype(out_type)


def line_phase(positions, location, length):
    turn_count = positions * location % length
    angles = turn_count.astype(jnp.float32) * (2.0 * math.pi / length)
    return (jnp.cos(angles), -jnp.sin(angles))


def complex_product(first, second):
    return jnp.stack(
        [first[0] * second[0] - first[1] * second[1], first[0] * second[1] + first[1] * second[0]]
    )


def forward(wave_field, dft_table):
    row_count, layer_count, grid_size = wave_field.shape[1:]
    narrowed = wave_field.astype(jnp.bfloat16)
    products = jnp.dot(
        narrowed.reshape(2 * row_count * layer_count, grid_size),
        dft_table,
        preferred_element_type=jnp.float32,
    )
    products = products.reshape(2, row_count, layer_count, 2, grid_size)
    real_part = products[0, :, :, 0] + products[1, :, :, 1]
    imag_part = products[1, :, :, 0] - products[0, :, :, 1]
    narrowed = jnp.stack([real_part, imag_part]).astype(jnp.bfloat16)
    arrived = lax.all_to_all(narrowed, "plane", split_axis=3, concat_axis=1, tiled=True)
    col_count = arrived.shape[3]
    merged = arrived.reshape(2, grid_size, layer_count * col_count)
    products = jnp.einsum("cxq,xk->cqk", merged, dft_table, preferred_element_type=jnp.float32)
    real_part = products[0, :, :grid_size] + products[1, :, grid_size:]
    imag_part = products[1, :, :grid_size] - products[0, :, grid_size:]
    return jnp.stack([real_part, imag_part]).reshape(2, layer_count, col_count, grid_size)


def inverse(spectrum, dft_table):
    layer_count, col_count, grid_size = spectrum.shape[1:]
    narrowed = spectrum.astype(jnp.bfloat16).reshape(2, layer_count * col_count, grid_size)
    products = jnp.einsum("cqk,kt->ctq", narrowed, dft_table, preferred_element_type=jnp.float32)
    real_part = products[0, :grid_size] - products[1, grid_size:]
    imag_part = products[1, :grid_size] + products[0, grid_size:]
    narrowed = (
        jnp.stack([real_part, imag_part])
        .astype(jnp.bfloat16)
        .reshape(2, grid_size, layer_count, col_count)
    )
    arrived = lax.all_to_all(narrowed, "plane", split_axis=1, concat_axis=3, tiled=True)
    row_count = arrived.shape[1]
    products = jnp.dot(
        arrived.reshape(2 * row_count * layer_count, grid_size),
        dft_table,
        preferred_element_type=jnp.float32,
    )
    products = products.reshape(2, row_count, layer_count, 2, grid_size)
    real_part = products[0, :, :, 0] - products[1, :, :, 1]
    imag_part = products[1, :, :, 0] + products[0, :, :, 1]
    return jnp.stack([real_part, imag_part])


def couple(spectrum, kernel):
    layer_count = spectrum.shape[1]
    real_rows = []
    imag_rows = []
    for out_layer in range(layer_count):
        sum_real = jnp.zeros(spectrum.shape[2:], jnp.float32)
        sum_imag = jnp.zeros(spectrum.shape[2:], jnp.float32)
        for in_layer in range(layer_count):
            kern_real = kernel[0, out_layer, in_layer].astype(jnp.float32)
            kern_imag = kernel[1, out_layer, in_layer].astype(jnp.float32)
            sum_real = (
                sum_real + kern_real * spectrum[0, in_layer] - kern_imag * spectrum[1, in_layer]
            )
            sum_imag = (
                sum_imag + kern_real * spectrum[1, in_layer] + kern_imag * spectrum[0, in_layer]
            )
        real_rows.append(sum_real)
        imag_rows.append(sum_imag)
    return jnp.stack([jnp.stack(real_rows), jnp.stack(imag_rows)])


def green_apply(wave_field, kernel, dft_table):
    return inverse(couple(forward(wave_field, dft_table), kernel), dft_table)


def plain_local(contrast, green_kernel, source_pos, receiver_pos, measured):
    freq_count = green_kernel.shape[0]
    row_count = contrast.shape[1]
    grid_size = contrast.shape[3]
    high = lax.Precision.HIGHEST
    dft_table = phase_tables(grid_size, jnp.bfloat16)
    first_row = lax.axis_index("plane") * row_count
    own_rows = first_row + lax.iota(jnp.int32, row_count)
    all_cols = lax.iota(jnp.int32, grid_size)
    which = 0
    kernel = green_kernel[which]
    phase_y_real, phase_y_imag = line_phase(own_rows, source_pos[which, 1], grid_size)
    phase_x_real, phase_x_imag = line_phase(all_cols, source_pos[which, 0], grid_size)
    source_real = source_gain * (
        phase_y_real[:, None] * phase_x_real[None, :]
        - phase_y_imag[:, None] * phase_x_imag[None, :]
    )
    source_imag = source_gain * (
        phase_y_real[:, None] * phase_x_imag[None, :]
        + phase_y_imag[:, None] * phase_x_real[None, :]
    )
    column_zero = kernel[:, :, 0].astype(jnp.float32)
    spectrum = jnp.stack(
        [
            column_zero[0] * source_real - column_zero[1] * source_imag,
            column_zero[0] * source_imag + column_zero[1] * source_real,
        ]
    )
    incident = inverse(spectrum, dft_table)
    wave_field = incident
    for sweep_index in range(ITERS):
        wave_field = incident + green_apply(
            complex_product(contrast, wave_field), kernel, dft_table
        )
    recv_x = receiver_pos[which, 0]
    recv_y = receiver_pos[which, 1]
    pick_rows = (recv_x[:, None] == own_rows[None, :]).astype(jnp.float32)
    pick_cols = (recv_y[:, None] == all_cols[None, :]).astype(jnp.float32)
    surface = jnp.einsum("rx,cxy->cry", pick_rows, wave_field[:, :, 0, :], precision=high)
    sampled = jnp.sum(surface * pick_cols[None], axis=2)
    gathered = lax.psum(sampled, "plane")
    misfit = gathered - measured[which]
    recv_y_real, recv_y_imag = line_phase(own_rows[None, :], recv_y[:, None], grid_size)
    recv_x_real, recv_x_imag = line_phase(all_cols[None, :], recv_x[:, None], grid_size)
    mixed_real = misfit[0][:, None] * recv_y_real - misfit[1][:, None] * recv_y_imag
    mixed_imag = misfit[0][:, None] * recv_y_imag + misfit[1][:, None] * recv_y_real
    contract = (((0,), (0,)), ((), ()))
    adj_real = lax.dot_general(
        mixed_real, recv_x_real, contract, precision=high, preferred_element_type=jnp.float32
    ) - lax.dot_general(
        mixed_imag, recv_x_imag, contract, precision=high, preferred_element_type=jnp.float32
    )
    adj_imag = lax.dot_general(
        mixed_real, recv_x_imag, contract, precision=high, preferred_element_type=jnp.float32
    ) + lax.dot_general(
        mixed_imag, recv_x_real, contract, precision=high, preferred_element_type=jnp.float32
    )
    row_zero = kernel[:, 0].astype(jnp.float32)
    back_spec = jnp.stack(
        [
            row_zero[0] * adj_real + row_zero[1] * adj_imag,
            row_zero[0] * adj_imag - row_zero[1] * adj_real,
        ]
    )
    backward = inverse(back_spec, dft_table)
    gradient = jnp.stack(
        [
            wave_field[0] * backward[0] + wave_field[1] * backward[1],
            wave_field[0] * backward[1] - wave_field[1] * backward[0],
        ]
    )
    incidents = [incident]
    solutions = [wave_field]
    total_freqs = freq_count * lax.axis_size("freq")
    summed = lax.psum(gradient.astype(jnp.bfloat16), "freq").astype(jnp.float32)
    updated = contrast - summed / total_freqs
    which = 0
    outputs = [
        incidents[which]
        + green_apply(complex_product(updated, solutions[which]), green_kernel[which], dft_table)
    ]
    return (updated, jnp.stack(outputs))


HIGH = lax.Precision.HIGHEST


def fused_kernel(
    cfg, con_in, kern_in, cos_t, sin_t, src_pos, recv_pos, measured,
    new_con, new_field,
    con, kt, rx, ry_real, ry_imag, pick_x, pick_y,
    tab_a, tab_b, inc, wave, back, vb, spec, hb, send_buf, recv_buf,
    samp_out, samp_in, grad, grad_b, half_in, part_out, part_in, total_b,
    send_sem, recv_sem, samp_send, samp_recv,
    one_send, one_recv, two_send, two_recv, three_send, three_recv, four_send, four_recv,
):
    n, nf, ck, layers, recv = cfg
    wide = 2 * ck
    length = n * ck
    quarter = length // 4
    nz = nf // 2
    me = lax.axis_index("plane")
    fr = lax.axis_index("freq")
    core = fr % 2
    z = fr // 2
    mate = fr + 1 - 2 * core

    def peer(k):
        if n == 4:
            return ((me // 2 + k // 2) % 2) * 2 + (me % 2 + k % 2) % 2
        return (me + k) % n

    def source(k):
        return peer(k) if n == 4 else (me + n - k) % n

    order = [3, 1, 2] if n == 4 else list(range(1, n))
    arrive = [1, 2, 3] if n == 4 else list(range(1, n))
    z_peers = [((z + 1 + j) % nz) * 2 + core for j in range(nz - 1)]

    barrier = pltpu.get_barrier_semaphore()
    for k in range(1, n):
        pl.semaphore_signal(barrier, inc=1, device_id={"plane": peer(k)})
    for dev in z_peers + [mate]:
        pl.semaphore_signal(barrier, inc=1, device_id={"freq": dev})

    def remote(src_ref, dst_ref, s, r, where):
        return pltpu.make_async_remote_copy(
            src_ref=src_ref, dst_ref=dst_ref, send_sem=s, recv_sem=r, device_id=where
        )

    def block(i):
        return pl.ds(pl.multiple_of(i * wide, wide), wide)

    def move(ph, k):
        return remote(
            send_buf.at[ph, k], recv_buf.at[ph, k], send_sem.at[ph, k], recv_sem.at[ph, k],
            {"plane": peer(k)},
        )

    for a in range(n):
        for b in range(n):
            cb = cos_t[a * ck : (a + 1) * ck, b * ck : (b + 1) * ck]
            sb = sin_t[a * ck : (a + 1) * ck, b * ck : (b + 1) * ck]
            r0, c0 = a * wide, b * wide
            for tab, up, down in ((tab_a, -sb, sb), (tab_b, sb, -sb)):
                tab[r0 : r0 + ck, c0 : c0 + ck] = cb
                tab[r0 : r0 + ck, c0 + ck : c0 + wide] = up
                tab[r0 + ck : r0 + wide, c0 : c0 + ck] = down
                tab[r0 + ck : r0 + wide, c0 + ck : c0 + wide] = cb

    def dot(a, b):
        return jnp.dot(a, b, preferred_element_type=jnp.float32)

    def turn_cos(turns):
        x = (turns & (length - 1)).astype(jnp.float32) * (math.pi / length) - math.pi / 2
        x2 = x * x
        s = -1.0 / 39916800.0
        for term in (1.0 / 362880.0, -1.0 / 5040.0, 1.0 / 120.0, -1.0 / 6.0, 1.0):
            s = term + x2 * s
        s = x * s
        return 2.0 * s * s - 1.0

    def iota(shape, axis):
        return lax.broadcasted_iota(jnp.int32, shape, axis)

    def strided(c, l, d):
        return pl.ds((c * ck * n + d) * layers + l, ck, stride=n * layers), slice(None)

    def flip(li):
        for c in range(2):
            for lo in range(layers):
                kt[c, lo, li] = kern_in[0, c, lo, li].T

    def prepare():
        for li in range(1, layers):
            flip(li)
        for c in range(2):
            for l in range(layers):
                for d in range(n):
                    at = d * wide + c * ck
                    con[l * ck : (l + 1) * ck, at : at + ck] = con_in[strided(c, l, d)]
        eye = iota((recv, recv), 0) == iota((recv, recv), 1)

        def column(row):
            return jnp.sum(jnp.where(eye, row, 0.0), axis=1, keepdims=True)

        places = recv_pos[0].astype(jnp.float32)
        x_col, y_col = column(places[0:1]), column(places[1:2])
        sub, lane = iota((recv, 2 * recv), 0), iota((recv, 2 * recv), 1)
        both = jnp.where((lane == sub) | (lane == sub + recv), x_col, 0.0)
        x_row = jnp.sum(both, axis=0, keepdims=True).astype(jnp.int32)
        x_col, y_col = x_col.astype(jnp.int32), y_col.astype(jnp.int32)
        late = iota((ck, 2 * recv), 1) >= recv
        for g in range(n):
            turns = (g * ck + iota((ck, 2 * recv), 0)) * x_row
            for c in range(2):
                shift = jnp.where(late, 0 if c else 3 * quarter, quarter if c else 0)
                rx[g * wide + c * ck : g * wide + (c + 1) * ck, :] = turn_cos(turns + shift)
            pick_y[:, g * ck : (g + 1) * ck] = (y_col == g * ck + iota((recv, ck), 1)).astype(
                jnp.float32
            )
        own = me * ck + iota((recv, ck), 1)
        pick_x[...] = (x_col == own).astype(jnp.float32)
        ry_real[...] = turn_cos(y_col * own)
        ry_imag[...] = turn_cos(y_col * own + quarter)
        return [column(measured[0, c : c + 1, :]) for c in range(2)]

    def forward(ph, beside=None):
        def piece(d):
            w = dot(vb[...], tab_a[:, block(d)]).astype(jnp.bfloat16)
            return [
                (c, l, w[l * ck : (l + 1) * ck, c * ck : (c + 1) * ck])
                for c in range(2)
                for l in range(layers)
            ]

        for k in order:
            for c, l, w in piece(peer(k)):
                send_buf[ph, k, c * ck : (c + 1) * ck, l * ck : (l + 1) * ck] = w
            move(ph, k).start()
        for c, l, w in piece(me):
            recv_buf[ph, 0, c * ck : (c + 1) * ck, l * ck : (l + 1) * ck] = w
        spec[...] = dot(tab_b[:, block(me)], recv_buf[ph, 0])
        if beside is not None:
            beside()
        for k in arrive:
            move(ph, k).wait_recv()
            spec[...] += dot(tab_b[:, block(source(k))], recv_buf[ph, k])
        for k in arrive:
            move(ph, k).wait_send()

    def inverse(ph, dst, base, beside=None):
        for k in order:
            send_buf[ph, k] = dot(tab_a[block(peer(k)), :], hb[...]).astype(jnp.bfloat16)
            move(ph, k).start()
        recv_buf[ph, 0] = dot(tab_a[block(me), :], hb[...]).astype(jnp.bfloat16)

        def part(k, s):
            p = recv_buf[ph, k]
            lhs = jnp.concatenate(
                [
                    jnp.concatenate(
                        [p[:ck, l * ck : (l + 1) * ck], p[ck:, l * ck : (l + 1) * ck]], axis=1
                    )
                    for l in range(layers)
                ],
                axis=0,
            )
            return dot(lhs, tab_b[block(s), :])

        dst[...] = part(0, me) if base is None else base[...] + part(0, me)
        kept = beside() if beside is not None else None
        for k in arrive:
            move(ph, k).wait_recv()
            dst[...] += part(k, source(k))
        for k in arrive:
            move(ph, k).wait_send()
        return kept

    def multiply(contrast_ref):
        for d in range(n):
            lo = slice(d * wide, d * wide + ck)
            hi = slice(d * wide + ck, (d + 1) * wide)
            a_r, a_i = contrast_ref[:, lo], contrast_ref[:, hi]
            u_r, u_i = wave[:, lo], wave[:, hi]
            vb[:, lo] = (a_r * u_r - a_i * u_i).astype(jnp.bfloat16)
            vb[:, hi] = (a_r * u_i + a_i * u_r).astype(jnp.bfloat16)

    def kern(c, lo, li, g):
        return kt[c, lo, li, g * ck : (g + 1) * ck, :].astype(jnp.float32)

    def put(g, l, real, imag):
        lanes = slice(l * ck, (l + 1) * ck)
        hb[g * wide : g * wide + ck, lanes] = real.astype(jnp.bfloat16)
        hb[g * wide + ck : (g + 1) * wide, lanes] = imag.astype(jnp.bfloat16)

    def couple():
        for g in range(n):
            for lo in range(layers):
                real = imag = None
                for li in range(layers):
                    lanes = slice(li * ck, (li + 1) * ck)
                    f_r = spec[g * wide : g * wide + ck, lanes]
                    f_i = spec[g * wide + ck : (g + 1) * wide, lanes]
                    k_r, k_i = kern(0, lo, li, g), kern(1, lo, li, g)
                    add_r = k_r * f_r - k_i * f_i
                    add_i = k_r * f_i + k_i * f_r
                    real = add_r if real is None else real + add_r
                    imag = add_i if imag is None else imag + add_i
                put(g, lo, real, imag)

    flip(0)
    for g in range(n):
        turns = (g * ck + iota((ck, ck), 0)) * src_pos[0, 0]
        turns = turns + (me * ck + iota((ck, ck), 1)) * src_pos[0, 1]
        q_r = source_gain * turn_cos(turns)
        q_i = source_gain * turn_cos(turns + quarter)
        for l in range(layers):
            k_r, k_i = kern(0, l, 0, g), kern(1, l, 0, g)
            put(g, l, k_r * q_r - k_i * q_i, k_r * q_i + k_i * q_r)

    pl.semaphore_wait(barrier, n - 1 + nz)

    meas_r, meas_i = inverse(0, inc, None, prepare)
    wave[...] = inc[...]

    def sweep(it, carry):
        multiply(con)
        forward(1 + 2 * it)
        couple()
        inverse(2 + 2 * it, wave, inc)
        return carry

    lax.fori_loop(0, ITERS, sweep, 0)
    ph = 1 + 2 * ITERS

    rows = jnp.dot(pick_x[...], wave[:ck, :], precision=HIGH, preferred_element_type=jnp.float32)
    got_r = got_i = None
    for d in range(n):
        mask = pick_y[:, d * ck : (d + 1) * ck]
        s_r = rows[:, d * wide : d * wide + ck] * mask
        s_i = rows[:, d * wide + ck : (d + 1) * wide] * mask
        got_r = s_r if d == 0 else got_r + s_r
        got_i = s_i if d == 0 else got_i + s_i
    got_r = jnp.sum(got_r, axis=1, keepdims=True)
    got_i = jnp.sum(got_i, axis=1, keepdims=True)
    samp_out[...] = jnp.where(iota(samp_out.shape, 1) < recv, got_r, got_i)

    def tell(k):
        return remote(
            samp_out, samp_in.at[k], samp_send.at[k], samp_recv.at[k], {"plane": peer(k)}
        )

    for k in order:
        tell(k).start()
    misfit = samp_out[...]
    for k in arrive:
        tell(k).wait_recv()
        misfit = misfit + samp_in[k]
    for k in arrive:
        tell(k).wait_send()
    m_r = misfit[:, 0:1] - meas_r
    m_i = misfit[:, recv : recv + 1] - meas_i
    y_r, y_i = ry_real[...], ry_imag[...]
    mixed = jnp.concatenate([m_r * y_r - m_i * y_i, m_r * y_i + m_i * y_r], axis=0)
    for g in range(n):
        adj = jnp.dot(
            rx[g * wide : (g + 1) * wide, :], mixed,
            precision=HIGH, preferred_element_type=jnp.float32,
        )
        a_r, a_i = adj[:ck], adj[ck:]
        for l in range(layers):
            k_r, k_i = kern(0, 0, l, g), kern(1, 0, l, g)
            put(g, l, k_r * a_r + k_i * a_i, k_r * a_i - k_i * a_r)
    inverse(ph, back, None)

    for d in range(n):
        lo = slice(d * wide, d * wide + ck)
        hi = slice(d * wide + ck, (d + 1) * wide)
        b_r, b_i, u_r, u_i = back[:, lo], back[:, hi], wave[:, lo], wave[:, hi]
        g_r = u_r * b_r + u_i * b_i
        g_i = u_r * b_i - u_i * b_r
        grad[:, lo] = g_r
        grad[:, hi] = g_i
        grad_b[:, lo] = g_r.astype(jnp.bfloat16)
        grad_b[:, hi] = g_i.astype(jnp.bfloat16)

    height = grad.shape[0] // 2
    q = height // nz

    def span(c, i):
        return pl.ds(pl.multiple_of(c * height + i * q, q), q)

    def first(j):
        t = (z + 1 + j) % nz
        return remote(
            grad_b.at[span(1 - core, t), :], half_in.at[j],
            one_send.at[j], one_recv.at[j], {"freq": mate},
        )

    def second(j):
        return remote(
            part_out.at[j], part_in.at[j], two_send.at[j], two_recv.at[j], {"freq": z_peers[j]}
        )

    for j in range(nz):
        first(j).start()
    mine = None
    for j in range(nz):
        t = (z + 1 + j) % nz
        first(j).wait_recv()
        mine = grad[span(core, t), :] + half_in[j].astype(jnp.float32)
        if j < nz - 1:
            part_out[j] = mine.astype(jnp.bfloat16)
            second(j).start()
    for j in range(nz - 1):
        second(j).wait_recv()
        mine = mine + part_in[j].astype(jnp.float32)
    total_b[span(core, z), :] = mine.astype(jnp.bfloat16)

    def third(j, i):
        rows_at = total_b.at[span(core, i), :]
        return remote(rows_at, rows_at, three_send.at[j], three_recv.at[j], {"freq": z_peers[j]})

    def fourth(j, c, i):
        rows_at = total_b.at[span(c, i), :]
        return remote(rows_at, rows_at, four_send.at[j], four_recv.at[j], {"freq": mate})

    for j in range(nz - 1):
        third(j, z).start()
    fourth(nz - 1, core, z).start()
    froms = [(z + nz - 1 - j) % nz for j in range(nz - 1)] + [z]
    for j in range(nz - 1):
        third(j, froms[j]).wait_recv()
        fourth(j, core, froms[j]).start()
    for j in reversed(range(nz)):
        fourth(j, 1 - core, froms[j]).wait_recv()
    for j in range(nz):
        first(j).wait_send()
        fourth(j, core, froms[j]).wait_send()
        if j < nz - 1:
            second(j).wait_send()
            third(j, z).wait_send()
    con[...] = con[...] - total_b[...].astype(jnp.float32) / nf

    def hand_out(out, values):
        for c in range(2):
            for l in range(layers):
                for d in range(n):
                    at = d * wide + c * ck
                    out[strided(c, l, d)] = values[l * ck : (l + 1) * ck, at : at + ck]

    multiply(con)
    forward(ph + 1, lambda: hand_out(new_con, con))
    couple()
    inverse(ph + 2, back, inc)
    hand_out(new_field, back)


def fused_local(contrast, green_kernel, source_pos, receiver_pos, measured):
    _, ck, layers, grid = contrast.shape
    n = lax.axis_size("plane")
    nf = lax.axis_size("freq")
    recv = receiver_pos.shape[2]
    wide = 2 * ck
    pos = np.arange(grid)
    ang = (pos[:, None] * pos[None, :] % grid) * (2.0 * math.pi / grid)
    cos_t = jnp.asarray((np.cos(ang) / math.sqrt(grid)).astype(np.float32).astype(jnp.bfloat16))
    sin_t = jnp.asarray((np.sin(ang) / math.sqrt(grid)).astype(np.float32).astype(jnp.bfloat16))
    con = contrast.reshape(2, ck, layers, n, ck).transpose(0, 1, 3, 2, 4)
    con = con.reshape(2 * ck * n * layers, ck)

    rows, cols, lanes = layers * ck, 2 * grid, layers * ck
    nz = nf // 2
    phases = 2 * ITERS + 4
    f32, bf16 = jnp.float32, jnp.bfloat16
    q = rows // 2 // nz
    dma = pltpu.SemaphoreType.DMA
    vm = pltpu.VMEM
    scratch = [
        vm((rows, cols), f32), vm((2, layers, layers, grid, ck), bf16), vm((cols, 2 * recv), f32),
        vm((recv, ck), f32), vm((recv, ck), f32), vm((recv, ck), f32), vm((recv, grid), f32),
        vm((cols, cols), bf16), vm((cols, cols), bf16), vm((rows, cols), f32),
        vm((rows, cols), f32), vm((rows, cols), f32), vm((rows, cols), bf16),
        vm((cols, lanes), f32), vm((cols, lanes), bf16),
        vm((phases, n, wide, lanes), bf16), vm((phases, n, wide, lanes), bf16),
        vm((recv, 2 * recv), f32), vm((n, recv, 2 * recv), f32),
        vm((rows, cols), f32), vm((rows, cols), bf16), vm((nz, q, cols), bf16),
        vm((nz - 1, q, cols), bf16), vm((nz - 1, q, cols), bf16), vm((rows, cols), bf16),
        dma((phases, n)), dma((phases, n)), dma((n,)), dma((n,)),
        dma((nz,)), dma((nz,)), dma((nz - 1,)), dma((nz - 1,)),
        dma((nz - 1,)), dma((nz - 1,)), dma((nz,)), dma((nz,)),
    ]
    spec = pl.BlockSpec(memory_space=pltpu.VMEM)
    new_con, new_field = pl.pallas_call(
        functools.partial(fused_kernel, (n, nf, ck, layers, recv)),
        out_shape=[jax.ShapeDtypeStruct(con.shape, f32)] * 2,
        in_specs=[spec] * 4 + [pl.BlockSpec(memory_space=pltpu.SMEM)] + [spec] * 2,
        out_specs=[spec] * 2,
        scratch_shapes=scratch,
        compiler_params=pltpu.CompilerParams(
            collective_id=0, has_side_effects=True, vmem_limit_bytes=56 * 2**20
        ),
    )(con, green_kernel, cos_t, sin_t, source_pos, receiver_pos, measured)

    def restore(values):
        values = values.reshape(2, ck, n, layers, ck).transpose(0, 1, 3, 2, 4)
        return values.reshape(2, ck, layers, grid)

    return restore(new_con), restore(new_field)[None]


def chosen(contrast, green_kernel, source_pos, receiver_pos, measured):
    ck = contrast.shape[1]
    nf = lax.axis_size("freq")
    grid = contrast.shape[3]
    fits = (
        ck == 128
        and green_kernel.shape[0] == 1
        and grid & (grid - 1) == 0
        and receiver_pos.shape[2] % 64 == 0
        and nf % 2 == 0
        and nf >= 4
        and (contrast.shape[2] * ck) % (16 * nf) == 0
        and lax.axis_size("plane") > 1
    )
    body = fused_local if fits else plain_local
    return body(contrast, green_kernel, source_pos, receiver_pos, measured)


def solution(mesh):
    return jax.shard_map(
        chosen,
        mesh=mesh,
        in_specs=(
            P(None, "plane", None, None),
            P("freq", None, None, None, "plane", None),
            P("freq", None),
            P("freq", None, None),
            P("freq", None, None),
        ),
        out_specs=(P(None, "plane", None, None), P("freq", None, "plane", None, None)),
        check_vma=False,
    )
```
